128 devices in a mesh: member: 32 (over x, y, core), lat: 4 (over z).
Axes of the slice: x: 4, y: 4, z: 4, core: 2. Of those that a mesh axis runs over, the one named last changes fastest.
Arguments:
- ensemble: float32 [64, 3, 1, 128, 1440], P('member', None, None, 'lat'), may hold values from -6 to 6
- observation: float32 [3, 1, 128, 1440], P(None, None, 'lat'), may hold values from -6 to 6
- valid_mask: int32 [64], P('member'), may hold values from 0 to 1, as said below
- band_start: int32 [4], P('lat'), may hold values from 0 to 689
Outputs:
- crps_field: float32 [3, 1, 128, 1440], P(None, None, ('lat', 'member'))
- score_table: float32 [3, 1], replicated
The draws below stay inside these ranges and needn't reach their ends.
Inputs may be any that keep to these rules, and one draw needn't show every extreme that they name: `valid_mask`: exactly 50 entries are 1, at positions drawn afresh.
All inputs are finite; a program needn't handle non-finite values.
Results may differ from the reference program's by a relative error of at most 0.0001.
Values sent between devices are 32-bit elements; how exact they have to be, the bound alone decides.
No kernel may reach another device: no remote copies, remote signals or barrier semaphores. Data moves between devices by JAX's collectives and lax.ppermute only.
A program may use at most 64 MiB of HBM per device.

```python
import math
import jax
import jax.numpy as jnp
from jax import lax

GRID_LAT = 721
GRID_LON = 1440
VARS = 3
LEADS = 1
LAT_DEV = 32
MEMBERS = 64
VALID = 50
LAT = 128
N_LAT = 4


def draw_valid_mask(key, part):
    shuffled = jax.random.permutation(jax.random.fold_in(key, 17), MEMBERS)
    return (shuffled < VALID).astype(jnp.int32)


def touch_ends(drawn, key, low, top_value):
    dims = drawn.shape
    spot = [jax.random.randint(jax.random.fold_in(key, axis), (), 0, dims[axis]) for axis in range(len(dims))]
    drawn = drawn.at[tuple(spot)].set(low)
    longest = dims.index(max(dims))
    spot[longest] = (spot[longest] + 1) % dims[longest]
    return drawn.at[tuple(spot)].set(top_value)


def steps_of(stream_key, shape, pieces, low, high):
    gain = 1.0
    for dim, shards_of in pieces:
        steps = jax.random.uniform(jax.random.fold_in(jax.random.fold_in(stream_key, 6), dim), (shards_of,), jnp.float32, low / len(pieces), high / len(pieces))
        gain = gain * jnp.repeat(jnp.exp(steps), shape[dim] // shards_of).reshape((-1,) + (1,) * (len(shape) - 1 - dim))
    return gain


def scatter_about(own_key, extent, scale, bound, split=(), kind=jnp.bfloat16):
    values = scale * jax.random.normal(own_key, extent, jnp.float32)
    if split:
        values = values * steps_of(own_key, extent, split, -0.22, 0.18)
    return jnp.clip(values, -bound, bound).astype(kind)


def setup_inputs(seed: int = 0) -> dict:
    arg_keys = jax.random.split(jax.random.key(seed), 5)
    return {
        "ensemble": scatter_about(arg_keys[0], (MEMBERS, VARS, LEADS, LAT, GRID_LON), 1.0, 6.0, ((0, 32), (3, 4)), jnp.float32),
        "observation": scatter_about(arg_keys[1], (VARS, LEADS, LAT, GRID_LON), 1.0, 6.0, ((2, 4),), jnp.float32),
        "valid_mask": draw_valid_mask(jax.random.fold_in(arg_keys[4], 71), 0),
        "band_start": touch_ends(jax.random.randint(arg_keys[3], (N_LAT,), 0, GRID_LAT - LAT_DEV + 1), jax.random.fold_in(arg_keys[3], 1), 0, GRID_LAT - LAT_DEV).astype(jnp.int32),
    }


def reference(ensemble, observation, valid_mask, band_start):
    member_flags = valid_mask.astype(jnp.float32)
    valid_count = jnp.sum(member_flags)
    flag_column = member_flags[:, None, None, None, None]
    skill_term = jnp.sum(flag_column * jnp.abs(ensemble - observation[None]), axis=0)

    def accumulate(running_sum, block_item):
        member_slab, member_flag = block_item
        distance = jnp.sum(flag_column * jnp.abs(member_slab[None] - ensemble), axis=0)
        return running_sum + member_flag * distance, None

    spread, unused = lax.scan(accumulate, jnp.zeros(observation.shape, jnp.float32), (ensemble, member_flags))
    crps_field = skill_term / valid_count - spread / (2.0 * valid_count * (valid_count - 1.0))
    row_index = (band_start[:, None] + jnp.arange(LAT_DEV, dtype=jnp.int32)[None, :]).reshape(-1).astype(jnp.float32)
    weight = jnp.cos((90.0 - row_index * 180.0 / (GRID_LAT - 1)) * math.pi / 180.0)
    score_table = jnp.sum(crps_field * weight[:, None], axis=(2, 3)) / (N_LAT * LAT_DEV * GRID_LON)
    return (crps_field, score_table)
```

```python
import math

import jax
import jax.numpy as jnp
from jax import lax
from jax.experimental import pallas as pl
from jax.experimental.pallas import tpu as pltpu
from jax.sharding import Mesh
from jax.sharding import PartitionSpec as P

GRID_LAT = 721
GRID_LON = 1440
LANES = 128
COLS = 12
VARS = 3
ROWS = 36
BLOCK = 72
MEMBERS = 64
VALID = 50
VMEM_LIMIT = 8 * 2**20
PAD = 1e30
MEMBER = ("member_0", "member_1", "member_2")
MEMBER_LAT = ("member_0", "member_1", "member_2", "lat")
LAT_MEMBER = ("lat", "member_0", "member_1", "member_2")


def slot(member, row):
    return 32 * member + row if row < 32 else 64 + 4 * member + row - 32


def pack_kernel(mask_ref, in_ref, out_ref):
    for member in range(2):
        valid = mask_ref[member] != 0
        for var in range(VARS):
            for col in range(COLS):
                low = col * LANES
                high = min(low + LANES, GRID_LON)
                piece = in_ref[member * VARS + var, :, low:high]
                if high - low < LANES:
                    fill = jnp.zeros((8, LANES - (high - low)), jnp.float32)
                    piece = jnp.concatenate([piece, fill], axis=1)
                piece = jnp.where(valid, piece, PAD)
                row = slot(member, var * COLS + col)
                out_ref[pl.ds(row, 8, stride=BLOCK), :] = piece


def pack(ensemble, valid_mask):
    rows = ensemble.shape[3]
    flat = ensemble.reshape(2 * VARS, rows, GRID_LON)
    packed = pl.pallas_call(
        pack_kernel,
        grid=(rows // 8,),
        in_specs=[
            pl.BlockSpec(memory_space=pltpu.SMEM),
            pl.BlockSpec((2 * VARS, 8, GRID_LON), lambda t: (0, t, 0)),
        ],
        out_specs=pl.BlockSpec((8 * BLOCK, LANES), lambda t: (t, 0)),
        out_shape=jax.ShapeDtypeStruct((rows * BLOCK, LANES), jnp.float32),
        name="pack",
    )(valid_mask, flat)
    return packed.reshape(rows, BLOCK, LANES)


def truth_kernel(row_ref, in_ref, out_ref):
    mine = lax.broadcasted_iota(jnp.int32, (8, LANES), 0) == row_ref[0] % 8
    out_ref[...] = jnp.zeros(out_ref.shape, jnp.float32)
    for var in range(VARS):
        for col in range(COLS):
            low = col * LANES
            high = min(low + LANES, GRID_LON)
            piece = jnp.where(mine[:, : high - low], in_ref[var, :, low:high], 0.0)
            row = var * COLS + col
            out_ref[row : row + 1, : high - low] = jnp.sum(piece, axis=0, keepdims=True)


def truth(observation, row):
    flat = observation.reshape(VARS, observation.shape[2], GRID_LON)
    return pl.pallas_call(
        truth_kernel,
        grid_spec=pltpu.PrefetchScalarGridSpec(
            num_scalar_prefetch=1,
            grid=(1,),
            in_specs=[pl.BlockSpec((VARS, 8, GRID_LON), lambda i, where: (0, where[0] // 8, 0))],
            out_specs=pl.BlockSpec((40, LANES), lambda i, where: (0, 0)),
        ),
        out_shape=jax.ShapeDtypeStruct((40, LANES), jnp.float32),
        compiler_params=pltpu.CompilerParams(vmem_limit_bytes=VMEM_LIMIT),
        name="truth",
    )(row.reshape(1), flat)


def compare(values, i, j):
    low, high = values[i], values[j]
    values[i] = jnp.minimum(low, high)
    values[j] = jnp.maximum(low, high)


def merge(values, where):
    if len(where) == 2:
        compare(values, where[0], where[1])
        return
    merge(values, where[0::2])
    merge(values, where[1::2])
    for k in range(1, len(where) - 1, 2):
        compare(values, where[k], where[k + 1])


def sort(values, where):
    if len(where) == 1:
        return
    half = len(where) // 2
    sort(values, where[:half])
    sort(values, where[half:])
    merge(values, where)


def score_of(ordered, observed):
    skill = sum(jnp.abs(v - observed) for v in ordered)
    spread = sum(
        (VALID - 1.0 - 2 * k) * (ordered[VALID - 1 - k] - ordered[k]) for k in range(VALID // 2)
    )
    return skill * (1.0 / VALID) - spread * (1.0 / (VALID * (VALID - 1.0)))


def score_kernel(weight_ref, in_ref, truth_ref, field_ref, sums_ref, field):
    @pl.loop(0, 4)
    def _(tile):
        start = pl.multiple_of(tile * 8, 8)
        values = []
        for source in range(MEMBERS // 2):
            values.append(in_ref[source, pl.ds(start, 8), :])
            values.append(in_ref[source, pl.ds(32 + start, 8), :])
        sort(values, list(range(MEMBERS)))
        field[pl.ds(start, 8), :] = score_of(values[:VALID], truth_ref[pl.ds(start, 8), :])

    half = MEMBERS // 2
    values = [in_ref[source, 64:72, :] for source in range(half)]
    sort(values, list(range(half)))
    upper = lax.broadcasted_iota(jnp.int32, (8, LANES), 0) >= 4
    other = [pltpu.roll(v, 4, 0) for v in values]
    values = [
        jnp.where(
            upper,
            jnp.maximum(values[k], other[half - 1 - k]),
            jnp.minimum(values[k], other[half - 1 - k]),
        )
        for k in range(half)
    ]
    step = half // 2
    while step:
        for k in range(half):
            if not k & step:
                compare(values, k, k + step)
        step //= 2
    above = [pltpu.roll(v, 4, 0) for v in values[: VALID - half]]
    field[32:40, :] = score_of(values + above, truth_ref[32:40, :])

    lane = lax.broadcasted_iota(jnp.int32, (1, LANES), 1)
    last = GRID_LON - (COLS - 1) * LANES
    sums = jnp.zeros((1, LANES), jnp.float32)
    for var in range(VARS):
        total = jnp.zeros((1, LANES), jnp.float32)
        for col in range(COLS):
            row = field[var * COLS + col : var * COLS + col + 1, :]
            low = col * LANES
            if col == COLS - 1:
                field_ref[var, :, low:GRID_LON] = row[:, :last]
                row = jnp.where(lane < last, row, 0.0)
            else:
                field_ref[var, :, low : low + LANES] = row
            total = total + row
        total = jnp.sum(total, axis=1, keepdims=True)
        sums = jnp.where(lane == var, total, sums)
    sums_ref[...] = jnp.broadcast_to(sums * weight_ref[0], sums_ref.shape)


def score(weight, members, observed, copies):
    return pl.pallas_call(
        score_kernel,
        in_specs=[
            pl.BlockSpec(memory_space=pltpu.SMEM),
            pl.BlockSpec(memory_space=pltpu.VMEM),
            pl.BlockSpec(memory_space=pltpu.VMEM),
        ],
        out_specs=[pl.BlockSpec(memory_space=pltpu.VMEM)] * 2,
        out_shape=[
            jax.ShapeDtypeStruct((VARS, 1, GRID_LON), jnp.float32),
            jax.ShapeDtypeStruct((copies, LANES), jnp.float32),
        ],
        scratch_shapes=[pltpu.VMEM((40, LANES), jnp.float32)],
        compiler_params=pltpu.CompilerParams(vmem_limit_bytes=VMEM_LIMIT),
        name="score",
    )(weight, members, observed)


def on_device(ensemble, observation, valid_mask, band_start):
    lat_rows = ensemble.shape[3]
    row = lax.axis_index(MEMBER).astype(jnp.int32)
    packed = pack(ensemble, valid_mask)
    members = lax.all_to_all(packed, MEMBER, split_axis=0, concat_axis=0, tiled=True)
    observed = truth(observation, row)
    place = (band_start + row).astype(jnp.float32)
    weight = jnp.cos((90.0 - place * 180.0 / (GRID_LAT - 1)) * math.pi / 180.0)
    copies = lax.axis_size(MEMBER_LAT)
    field, sums = score(weight, members, observed, copies)
    sums = lax.all_to_all(sums, MEMBER_LAT, split_axis=0, concat_axis=0, tiled=True)
    total = jnp.sum(sums, axis=0)[:VARS].reshape(VARS, 1)
    score_table = total / (lax.axis_size("lat") * lat_rows * GRID_LON)
    return (field.reshape(VARS, 1, 1, GRID_LON), score_table)


def solution(mesh):
    torus = Mesh(
        mesh.devices.reshape(4, 4, 2, mesh.shape["lat"]),
        ("member_0", "member_1", "member_2", "lat"),
    )
    in_specs = (P(MEMBER, None, None, "lat", None), P(None, None, "lat", None), P(MEMBER), P("lat"))
    out_specs = (P(None, None, LAT_MEMBER, None), P())
    return jax.shard_map(
        on_device, mesh=torus, in_specs=in_specs, out_specs=out_specs, check_vma=False
    )
```

```python
import functools
import math

import jax
import jax.numpy as jnp
from jax import lax
from jax.experimental import pallas as pl
from jax.experimental.pallas import tpu as pltpu
from jax.sharding import Mesh
from jax.sharding import PartitionSpec as P

GRID_LAT = 721
GRID_LON = 1440
LANES = 128
COLS = 12
VARS = 3
ROWS = 36
BLOCK = 72
MEMBERS = 64
VALID = 50
VMEM_LIMIT = 8 * 2**20
PAD = 1e30
MEMBER = ("member_0", "member_1", "member_2")
MEMBER_LAT = ("member_0", "member_1", "member_2", "lat")
LAT_MEMBER = ("lat", "member_0", "member_1", "member_2")


def slot(member, row):
    return 32 * member + row if row < 32 else 64 + 4 * member + row - 32


def position():
    return lax.axis_index(MEMBER).astype(jnp.int32)


def in_hbm(x):
    return pltpu.with_memory_space_constraint(x, pltpu.HBM)


def pack_kernel(mask_in, in_ref, out_ref, mask_ref, held, packed, arrived, left):
    tiles = held.shape[1] // 8
    depth = 8 * BLOCK

    def bring(tile):
        rows = pl.ds(tile * 8, 8)
        return pltpu.make_async_copy(
            in_ref.at[:, rows, :], held.at[:, rows, :], arrived.at[tile]
        )

    def take(tile):
        rows = pl.ds(tile * depth, depth)
        return pltpu.make_async_copy(packed.at[rows, :], out_ref.at[rows, :], left.at[tile])

    flags = pltpu.make_async_copy(mask_in, mask_ref, arrived.at[tiles])
    flags.start()
    for tile in range(tiles):
        bring(tile).start()
    flags.wait()
    for tile in range(tiles):
        bring(tile).wait()
        for member in range(2):
            valid = mask_ref[member] != 0
            for var in range(VARS):
                for col in range(COLS):
                    low = col * LANES
                    high = min(low + LANES, GRID_LON)
                    piece = held[member * VARS + var, tile * 8 : tile * 8 + 8, low:high]
                    if high - low < LANES:
                        fill = jnp.zeros((8, LANES - (high - low)), jnp.float32)
                        piece = jnp.concatenate([piece, fill], axis=1)
                    piece = jnp.where(valid, piece, PAD)
                    start = tile * depth + slot(member, var * COLS + col)
                    packed[pl.ds(start, 8, stride=BLOCK), :] = piece
        take(tile).start()
    for tile in range(tiles):
        take(tile).wait()


def pack(ensemble, valid_mask):
    rows = ensemble.shape[3]
    packed = pl.pallas_call(
        pack_kernel,
        in_specs=[pl.BlockSpec(memory_space=pltpu.HBM)] * 2,
        out_specs=pl.BlockSpec(memory_space=pltpu.HBM),
        out_shape=jax.ShapeDtypeStruct((rows * BLOCK, LANES), jnp.float32),
        scratch_shapes=[
            pltpu.SMEM((2,), jnp.int32),
            pltpu.VMEM((2 * VARS, rows, GRID_LON), jnp.float32),
            pltpu.VMEM((rows * BLOCK, LANES), jnp.float32),
            pltpu.SemaphoreType.DMA((rows // 8 + 1,)),
            pltpu.SemaphoreType.DMA((rows // 8,)),
        ],
        compiler_params=pltpu.CompilerParams(vmem_limit_bytes=VMEM_LIMIT),
        name="pack",
    )(in_hbm(valid_mask), in_hbm(ensemble.reshape(2 * VARS, rows, GRID_LON)))
    return packed.reshape(rows, BLOCK, LANES)


def truth_kernel(start_ref, in_ref, truth_ref, weight_ref, near, arrived):
    row = position()
    around = pl.ds(pl.multiple_of((row // 8) * 8, 8), 8)
    look = pltpu.make_async_copy(in_ref.at[:, around, :], near, arrived)
    look.start()
    place = jnp.full((8, LANES), start_ref[0] + row, jnp.int32).astype(jnp.float32)
    angle = (90.0 - place * 180.0 / (GRID_LAT - 1)) * math.pi / 180.0
    weight_ref[...] = jnp.cos(angle)
    mine = lax.broadcasted_iota(jnp.int32, (8, LANES), 0) == row % 8
    truth_ref[...] = jnp.zeros(truth_ref.shape, jnp.float32)
    look.wait()
    for var in range(VARS):
        for col in range(COLS):
            low = col * LANES
            high = min(low + LANES, GRID_LON)
            piece = jnp.where(mine[:, : high - low], near[var, :, low:high], 0.0)
            to = var * COLS + col
            truth_ref[to : to + 1, : high - low] = jnp.sum(piece, axis=0, keepdims=True)


def truth(observation, band_start):
    rows = observation.shape[2]
    return pl.pallas_call(
        truth_kernel,
        in_specs=[
            pl.BlockSpec(memory_space=pltpu.SMEM),
            pl.BlockSpec(memory_space=pltpu.HBM),
        ],
        out_specs=[pl.BlockSpec(memory_space=pltpu.VMEM)] * 2,
        out_shape=[
            jax.ShapeDtypeStruct((40, LANES), jnp.float32),
            jax.ShapeDtypeStruct((8, LANES), jnp.float32),
        ],
        scratch_shapes=[
            pltpu.VMEM((VARS, 8, GRID_LON), jnp.float32),
            pltpu.SemaphoreType.DMA(()),
        ],
        compiler_params=pltpu.CompilerParams(vmem_limit_bytes=VMEM_LIMIT),
        name="truth",
    )(band_start, in_hbm(observation.reshape(VARS, rows, GRID_LON)))


def compare(values, i, j):
    low, high = values[i], values[j]
    values[i] = jnp.minimum(low, high)
    values[j] = jnp.maximum(low, high)


def merge(values, where):
    if len(where) == 2:
        compare(values, where[0], where[1])
        return
    merge(values, where[0::2])
    merge(values, where[1::2])
    for k in range(1, len(where) - 1, 2):
        compare(values, where[k], where[k + 1])


def sort(values, where):
    if len(where) == 1:
        return
    half = len(where) // 2
    sort(values, where[:half])
    sort(values, where[half:])
    merge(values, where)


def score_of(ordered, observed):
    skill = sum(jnp.abs(v - observed) for v in ordered)
    spread = sum(
        (VALID - 1.0 - 2 * k) * (ordered[VALID - 1 - k] - ordered[k]) for k in range(VALID // 2)
    )
    return skill * (1.0 / VALID) - spread * (1.0 / (VALID * (VALID - 1.0)))


def score_kernel(weight_ref, in_ref, truth_ref, field_ref, sums_ref, field):
    @pl.loop(0, 4)
    def _(tile):
        start = pl.multiple_of(tile * 8, 8)
        values = []
        for source in range(MEMBERS // 2):
            values.append(in_ref[source, pl.ds(start, 8), :])
            values.append(in_ref[source, pl.ds(32 + start, 8), :])
        sort(values, list(range(MEMBERS)))
        field[pl.ds(start, 8), :] = score_of(values[:VALID], truth_ref[pl.ds(start, 8), :])

    half = MEMBERS // 2
    values = [in_ref[source, 64:72, :] for source in range(half)]
    sort(values, list(range(half)))
    upper = lax.broadcasted_iota(jnp.int32, (8, LANES), 0) >= 4
    other = [pltpu.roll(v, 4, 0) for v in values]
    values = [
        jnp.where(
            upper,
            jnp.maximum(values[k], other[half - 1 - k]),
            jnp.minimum(values[k], other[half - 1 - k]),
        )
        for k in range(half)
    ]
    step = half // 2
    while step:
        for k in range(half):
            if not k & step:
                compare(values, k, k + step)
        step //= 2
    above = [pltpu.roll(v, 4, 0) for v in values[: VALID - half]]
    field[32:40, :] = score_of(values + above, truth_ref[32:40, :])

    lane = lax.broadcasted_iota(jnp.int32, (1, LANES), 1)
    last = GRID_LON - (COLS - 1) * LANES
    sums = jnp.zeros((1, LANES), jnp.float32)
    for var in range(VARS):
        total = jnp.zeros((1, LANES), jnp.float32)
        for col in range(COLS):
            row = field[var * COLS + col : var * COLS + col + 1, :]
            low = col * LANES
            if col == COLS - 1:
                field_ref[var, :, low:GRID_LON] = row[:, :last]
                row = jnp.where(lane < last, row, 0.0)
            else:
                field_ref[var, :, low : low + LANES] = row
            total = total + row
        total = jnp.sum(total, axis=1, keepdims=True)
        sums = jnp.where(lane == var, total, sums)
    sums_ref[...] = jnp.broadcast_to(sums * weight_ref[0:1, :], sums_ref.shape)


def score(weight, members, observed, copies):
    return pl.pallas_call(
        score_kernel,
        in_specs=[
            pl.BlockSpec(memory_space=pltpu.VMEM),
            pl.BlockSpec(memory_space=pltpu.VMEM),
            pl.BlockSpec(memory_space=pltpu.VMEM),
        ],
        out_specs=[pl.BlockSpec(memory_space=pltpu.VMEM)] * 2,
        out_shape=[
            jax.ShapeDtypeStruct((VARS, 1, GRID_LON), jnp.float32),
            jax.ShapeDtypeStruct((copies, LANES), jnp.float32),
        ],
        scratch_shapes=[pltpu.VMEM((40, LANES), jnp.float32)],
        compiler_params=pltpu.CompilerParams(vmem_limit_bytes=VMEM_LIMIT),
        name="score",
    )(weight, members, observed)


def finish_kernel(in_ref, ready_ref, table_ref, field_ref, table, sent, *, cells):
    first = pltpu.make_async_copy(ready_ref, field_ref, sent.at[0])
    second = pltpu.make_async_copy(table, table_ref, sent.at[1])
    first.start()
    table[...] = jnp.sum(in_ref[...], axis=0, keepdims=True)[:, :VARS] / cells
    second.start()
    first.wait()
    second.wait()


def finish(sums, field, cells):
    return pl.pallas_call(
        functools.partial(finish_kernel, cells=cells),
        in_specs=[pl.BlockSpec(memory_space=pltpu.VMEM)] * 2,
        out_specs=[pl.BlockSpec(memory_space=pltpu.HBM)] * 2,
        out_shape=[
            jax.ShapeDtypeStruct((1, VARS), jnp.float32),
            jax.ShapeDtypeStruct(field.shape, jnp.float32),
        ],
        scratch_shapes=[pltpu.VMEM((1, VARS), jnp.float32), pltpu.SemaphoreType.DMA((2,))],
        compiler_params=pltpu.CompilerParams(vmem_limit_bytes=VMEM_LIMIT),
        name="finish",
    )(sums, field)


def on_device(ensemble, observation, valid_mask, band_start):
    lat_rows = ensemble.shape[3]
    packed = pack(ensemble, valid_mask)
    members = lax.all_to_all(packed, MEMBER, split_axis=0, concat_axis=0, tiled=True)
    observed, weight = truth(observation, band_start)
    field, sums = score(weight, members, observed, lax.axis_size(MEMBER_LAT))
    sums = lax.all_to_all(sums, MEMBER_LAT, split_axis=0, concat_axis=0, tiled=True)
    cells = lax.axis_size("lat") * lat_rows * GRID_LON
    table, field = finish(sums, field, cells)
    return (field.reshape(VARS, 1, 1, GRID_LON), table.reshape(VARS, 1))


def solution(mesh):
    torus = Mesh(
        mesh.devices.reshape(4, 4, 2, mesh.shape["lat"]),
        ("member_0", "member_1", "member_2", "lat"),
    )
    in_specs = (P(MEMBER, None, None, "lat", None), P(None, None, "lat", None), P(MEMBER), P("lat"))
    out_specs = (P(None, None, LAT_MEMBER, None), P())
    return jax.shard_map(
        on_device, mesh=torus, in_specs=in_specs, out_specs=out_specs, check_vma=False
    )
```

```python
import functools
import math

import jax
import jax.numpy as jnp
from jax import lax
from jax.experimental import pallas as pl
from jax.experimental.pallas import tpu as pltpu
from jax.sharding import Mesh
from jax.sharding import PartitionSpec as P

GRID_LAT = 721
GRID_LON = 1440
LANES = 128
VARS = 3
FULL = 11
TAIL = 32
BLOCK = 68
WHOLE = 32
MEMBERS = 64
VALID = 50
VMEM_LIMIT = 8 * 2**20
PAD = 1e30
MEMBER = ("member_0", "member_1", "member_2")
MEMBER_LAT = ("member_0", "member_1", "member_2", "lat")
LAT_MEMBER = ("lat", "member_0", "member_1", "member_2")


def position():
    return lax.axis_index(MEMBER).astype(jnp.int32)


def in_hbm(x):
    return pltpu.with_memory_space_constraint(x, pltpu.HBM)


def pack_kernel(mask_in, in_ref, out_ref, mask_ref, held, packed, arrived, left):
    tiles = held.shape[1] // 8
    depth = 8 * BLOCK
    core = lax.axis_index(MEMBER[2]).astype(jnp.int32)

    def bring(tile):
        rows = pl.ds(tile * 8, 8)
        return pltpu.make_async_copy(
            in_ref.at[:, rows, :], held.at[:, rows, :], arrived.at[tile]
        )

    def take(tile):
        rows = pl.ds(tile * depth, depth)
        return pltpu.make_async_copy(packed.at[rows, :], out_ref.at[rows, :], left.at[tile])

    flags = pltpu.make_async_copy(mask_in, mask_ref, arrived.at[tiles])
    flags.start()
    for tile in range(tiles):
        bring(tile).start()
    flags.wait()
    for tile in range(tiles):
        bring(tile).wait()
        rows = slice(tile * 8, tile * 8 + 8)
        for member in range(2):
            valid = mask_ref[member] != 0
            pieces = []
            ends = []
            for var in range(VARS):
                for col in range(FULL):
                    low = col * LANES
                    pieces.append(held[member * VARS + var, rows, low : low + LANES])
                ends.append(held[member * VARS + var, rows, FULL * LANES : GRID_LON])
            ends.append(jnp.zeros((8, LANES - VARS * TAIL), jnp.float32))
            pieces.append(jnp.concatenate(ends, axis=1))
            for row, piece in enumerate(pieces):
                piece = jnp.where(valid, piece, PAD)
                if row < WHOLE:
                    start = tile * depth + 4 * core + WHOLE * member + row
                else:
                    start = tile * depth + 64 * (1 - core) + 2 * member + row - WHOLE
                packed[pl.ds(start, 8, stride=BLOCK), :] = piece
        take(tile).start()
    for tile in range(tiles):
        take(tile).wait()


def pack(ensemble, valid_mask):
    rows = ensemble.shape[3]
    packed = pl.pallas_call(
        pack_kernel,
        in_specs=[pl.BlockSpec(memory_space=pltpu.HBM)] * 2,
        out_specs=pl.BlockSpec(memory_space=pltpu.HBM),
        out_shape=jax.ShapeDtypeStruct((rows * BLOCK, LANES), jnp.float32),
        scratch_shapes=[
            pltpu.SMEM((2,), jnp.int32),
            pltpu.VMEM((2 * VARS, rows, GRID_LON), jnp.float32),
            pltpu.VMEM((rows * BLOCK, LANES), jnp.float32),
            pltpu.SemaphoreType.DMA((rows // 8 + 1,)),
            pltpu.SemaphoreType.DMA((rows // 8,)),
        ],
        compiler_params=pltpu.CompilerParams(vmem_limit_bytes=VMEM_LIMIT),
        name="pack",
    )(in_hbm(valid_mask), in_hbm(ensemble.reshape(2 * VARS, rows, GRID_LON)))
    return packed.reshape(rows, BLOCK // 4, 4, LANES)


def truth_kernel(start_ref, in_ref, truth_ref, weight_ref, near, arrived):
    row = position()
    around = pl.ds(pl.multiple_of((row // 8) * 8, 8), 8)
    look = pltpu.make_async_copy(in_ref.at[:, around, :], near, arrived)
    look.start()
    place = jnp.full((8, LANES), start_ref[0] + row, jnp.int32).astype(jnp.float32)
    angle = (90.0 - place * 180.0 / (GRID_LAT - 1)) * math.pi / 180.0
    weight_ref[...] = jnp.cos(angle)
    mine = lax.broadcasted_iota(jnp.int32, (8, LANES), 0) == row % 8
    look.wait()

    def pick(var, low, high):
        piece = jnp.where(mine[:, : high - low], near[var, :, low:high], 0.0)
        return jnp.sum(piece, axis=0, keepdims=True)

    rows = [
        pick(var, col * LANES, col * LANES + LANES) for var in range(VARS) for col in range(FULL)
    ]
    ends = [pick(var, FULL * LANES, GRID_LON) for var in range(VARS)]
    ends.append(jnp.zeros((1, LANES - VARS * TAIL), jnp.float32))
    rows.append(jnp.concatenate(ends, axis=1))
    for row in range(WHOLE):
        truth_ref[row : row + 1, :] = rows[row]
    for row in range(8):
        truth_ref[WHOLE + row : WHOLE + row + 1, :] = rows[WHOLE + row % 2]


def truth(observation, band_start):
    rows = observation.shape[2]
    return pl.pallas_call(
        truth_kernel,
        in_specs=[
            pl.BlockSpec(memory_space=pltpu.SMEM),
            pl.BlockSpec(memory_space=pltpu.HBM),
        ],
        out_specs=[pl.BlockSpec(memory_space=pltpu.VMEM)] * 2,
        out_shape=[
            jax.ShapeDtypeStruct((40, LANES), jnp.float32),
            jax.ShapeDtypeStruct((8, LANES), jnp.float32),
        ],
        scratch_shapes=[
            pltpu.VMEM((VARS, 8, GRID_LON), jnp.float32),
            pltpu.SemaphoreType.DMA(()),
        ],
        compiler_params=pltpu.CompilerParams(vmem_limit_bytes=VMEM_LIMIT),
        name="truth",
    )(band_start, in_hbm(observation.reshape(VARS, rows, GRID_LON)))


def compare(values, i, j):
    low, high = values[i], values[j]
    values[i] = jnp.minimum(low, high)
    values[j] = jnp.maximum(low, high)


def merge(values, where):
    if len(where) == 2:
        compare(values, where[0], where[1])
        return
    merge(values, where[0::2])
    merge(values, where[1::2])
    for k in range(1, len(where) - 1, 2):
        compare(values, where[k], where[k + 1])


def sort(values, where):
    if len(where) == 1:
        return
    half = len(where) // 2
    sort(values, where[:half])
    sort(values, where[half:])
    merge(values, where)


def score_of(ordered, observed):
    skill = sum(jnp.abs(v - observed) for v in ordered)
    spread = sum(
        (VALID - 1.0 - 2 * k) * (ordered[VALID - 1 - k] - ordered[k]) for k in range(VALID // 2)
    )
    return skill * (1.0 / VALID) - spread * (1.0 / (VALID * (VALID - 1.0)))


def halve(values):
    step = len(values) // 2
    while step:
        for k in range(len(values)):
            if not k & step:
                compare(values, k, k + step)
        step //= 2


def score_rest(parts, observed):
    count = len(parts)
    sublane = lax.broadcasted_iota(jnp.int32, (8, LANES), 0)
    pair = sublane // 2
    odd = pair % 2 == 1
    upper = pair >= 2
    values = list(parts)

    def swap(v, beside):
        up, down = pltpu.roll(v, 2, 0), pltpu.roll(v, 6, 0)
        return jnp.where(odd, up, down) if beside else jnp.where(odd, down, up)

    def split(values, others, high):
        return [
            jnp.where(high, jnp.maximum(v, w), jnp.minimum(v, w)) for v, w in zip(values, others)
        ]

    sort(values, list(range(count)))
    values = split(values, [swap(v, True) for v in values[::-1]], odd)
    halve(values)
    values = split(values, [swap(v, False) for v in values[::-1]], upper)
    values = split(values, [swap(v, True) for v in values], odd)
    halve(values)
    skill = jnp.zeros((8, LANES), jnp.float32)
    spread = jnp.zeros((8, LANES), jnp.float32)
    for k, v in enumerate(values):
        rank = count * pair + k
        v = jnp.where(rank < VALID, v, observed)
        weight = jnp.where(rank < VALID, 2 * rank - (VALID - 1), 0).astype(jnp.float32)
        skill = skill + jnp.abs(v - observed)
        spread = spread + weight * v
    total = skill * (1.0 / VALID) - spread * (1.0 / (VALID * (VALID - 1.0)))
    total = total + pltpu.roll(total, 4, 0)
    return total + pltpu.roll(total, 2, 0)


def score_kernel(weight_ref, in_ref, truth_ref, field_ref, sums_ref, field):
    sources = MEMBERS // 2

    @pl.loop(0, WHOLE // 8)
    def _(tile):
        values = []
        for source in range(sources):
            for member in range(2):
                base = BLOCK * source + 4 * (source % 2) + WHOLE * member
                at = pl.multiple_of(base + tile * 8, 8)
                values.append(in_ref[pl.ds(at, 8), :])
        sort(values, list(range(MEMBERS)))
        start = pl.multiple_of(tile * 8, 8)
        field[pl.ds(start, 8), :] = score_of(values[:VALID], truth_ref[pl.ds(start, 8), :])

    parts = [in_ref[136 * k + 64 : 136 * k + 72, :] for k in range(sources // 2)]
    field[WHOLE : WHOLE + 8, :] = score_rest(parts, truth_ref[WHOLE : WHOLE + 8, :])

    lane = lax.broadcasted_iota(jnp.int32, (1, LANES), 1)
    ends = field[VARS * FULL : VARS * FULL + 1, :]
    sums = jnp.zeros((1, LANES), jnp.float32)
    for var in range(VARS):
        total = jnp.where((lane >= var * TAIL) & (lane < (var + 1) * TAIL), ends, 0.0)
        for col in range(FULL):
            row = field[var * FULL + col : var * FULL + col + 1, :]
            field_ref[var, :, col * LANES : col * LANES + LANES] = row
            total = total + row
        field_ref[var, :, FULL * LANES : GRID_LON] = ends[:, var * TAIL : (var + 1) * TAIL]
        total = jnp.sum(total, axis=1, keepdims=True)
        sums = jnp.where(lane == var, total, sums)
    sums_ref[...] = jnp.broadcast_to(sums * weight_ref[0:1, :], sums_ref.shape)


def score(weight, members, observed, copies):
    return pl.pallas_call(
        score_kernel,
        in_specs=[
            pl.BlockSpec(memory_space=pltpu.VMEM),
            pl.BlockSpec(memory_space=pltpu.VMEM),
            pl.BlockSpec(memory_space=pltpu.VMEM),
        ],
        out_specs=[pl.BlockSpec(memory_space=pltpu.VMEM)] * 2,
        out_shape=[
            jax.ShapeDtypeStruct((VARS, 1, GRID_LON), jnp.float32),
            jax.ShapeDtypeStruct((copies, LANES), jnp.float32),
        ],
        scratch_shapes=[pltpu.VMEM((40, LANES), jnp.float32)],
        compiler_params=pltpu.CompilerParams(vmem_limit_bytes=VMEM_LIMIT),
        name="score",
    )(weight, members, observed)


def finish_kernel(in_ref, ready_ref, table_ref, field_ref, table, sent, *, cells):
    first = pltpu.make_async_copy(ready_ref, field_ref, sent.at[0])
    second = pltpu.make_async_copy(table, table_ref, sent.at[1])
    first.start()
    table[...] = jnp.sum(in_ref[...], axis=0, keepdims=True)[:, :VARS] / cells
    second.start()
    first.wait()
    second.wait()


def finish(sums, field, cells):
    return pl.pallas_call(
        functools.partial(finish_kernel, cells=cells),
        in_specs=[pl.BlockSpec(memory_space=pltpu.VMEM)] * 2,
        out_specs=[pl.BlockSpec(memory_space=pltpu.HBM)] * 2,
        out_shape=[
            jax.ShapeDtypeStruct((1, VARS), jnp.float32),
            jax.ShapeDtypeStruct(field.shape, jnp.float32),
        ],
        scratch_shapes=[pltpu.VMEM((1, VARS), jnp.float32), pltpu.SemaphoreType.DMA((2,))],
        compiler_params=pltpu.CompilerParams(vmem_limit_bytes=VMEM_LIMIT),
        name="finish",
    )(sums, field)


def on_device(ensemble, observation, valid_mask, band_start):
    lat_rows = ensemble.shape[3]
    packed = pack(ensemble, valid_mask)
    members = lax.all_to_all(packed, MEMBER, split_axis=0, concat_axis=0, tiled=True)
    members = members.reshape(-1, LANES)
    observed, weight = truth(observation, band_start)
    field, sums = score(weight, members, observed, lax.axis_size(MEMBER_LAT))
    sums = lax.all_to_all(sums, MEMBER_LAT, split_axis=0, concat_axis=0, tiled=True)
    cells = lax.axis_size("lat") * lat_rows * GRID_LON
    table, field = finish(sums, field, cells)
    return (field.reshape(VARS, 1, 1, GRID_LON), table.reshape(VARS, 1))


def solution(mesh):
    torus = Mesh(
        mesh.devices.reshape(4, 4, 2, mesh.shape["lat"]),
        ("member_0", "member_1", "member_2", "lat"),
    )
    in_specs = (P(MEMBER, None, None, "lat", None), P(None, None, "lat", None), P(MEMBER), P("lat"))
    out_specs = (P(None, None, LAT_MEMBER, None), P())
    return jax.shard_map(
        on_device, mesh=torus, in_specs=in_specs, out_specs=out_specs, check_vma=False
    )
```

```python
import functools
import math

import jax
import jax.numpy as jnp
from jax import lax
from jax.experimental import pallas as pl
from jax.experimental.pallas import tpu as pltpu
from jax.sharding import Mesh
from jax.sharding import PartitionSpec as P

GRID_LAT = 721
GRID_LON = 1440
LANES = 128
VARS = 3
FULL = 11
TAIL = 32
BLOCK = 68
WHOLE = 32
MEMBERS = 64
VALID = 50
VMEM_LIMIT = 8 * 2**20
PAD = 1e30
MEMBER = ("member_0", "member_1", "member_2")
MEMBER_LAT = ("member_2", "member_0", "member_1", "lat")
LAT_MEMBER = ("lat", "member_0", "member_1", "member_2")


def position():
    return lax.axis_index(MEMBER).astype(jnp.int32)


def in_hbm(x):
    return pltpu.with_memory_space_constraint(x, pltpu.HBM)


def pack_kernel(mask_in, in_ref, out_ref, mask_ref, held, packed, arrived, left):
    tiles = held.shape[1] // 8
    depth = 8 * BLOCK
    core = lax.axis_index(MEMBER[2]).astype(jnp.int32)

    def bring(tile):
        rows = pl.ds(tile * 8, 8)
        return pltpu.make_async_copy(
            in_ref.at[:, rows, :], held.at[:, rows, :], arrived.at[tile]
        )

    def take(tile):
        rows = pl.ds(tile * depth, depth)
        return pltpu.make_async_copy(packed.at[rows, :], out_ref.at[rows, :], left.at[tile])

    flags = pltpu.make_async_copy(mask_in, mask_ref, arrived.at[tiles])
    flags.start()
    for tile in range(tiles):
        bring(tile).start()
    flags.wait()
    for tile in range(tiles):
        bring(tile).wait()
        rows = slice(tile * 8, tile * 8 + 8)
        for member in range(2):
            valid = mask_ref[member] != 0
            pieces = []
            ends = []
            for var in range(VARS):
                for col in range(FULL):
                    low = col * LANES
                    pieces.append(held[member * VARS + var, rows, low : low + LANES])
                ends.append(held[member * VARS + var, rows, FULL * LANES : GRID_LON])
            ends.append(jnp.zeros((8, LANES - VARS * TAIL), jnp.float32))
            pieces.append(jnp.concatenate(ends, axis=1))
            for row, piece in enumerate(pieces):
                piece = jnp.where(valid, piece, PAD)
                if row < WHOLE:
                    start = tile * depth + 4 * core + WHOLE * member + row
                else:
                    start = tile * depth + 64 * (1 - core) + 2 * member + row - WHOLE
                packed[pl.ds(start, 8, stride=BLOCK), :] = piece
        take(tile).start()
    for tile in range(tiles):
        take(tile).wait()


def pack(ensemble, valid_mask):
    rows = ensemble.shape[3]
    packed = pl.pallas_call(
        pack_kernel,
        in_specs=[pl.BlockSpec(memory_space=pltpu.HBM)] * 2,
        out_specs=pl.BlockSpec(memory_space=pltpu.HBM),
        out_shape=jax.ShapeDtypeStruct((rows * BLOCK, LANES), jnp.float32),
        scratch_shapes=[
            pltpu.SMEM((2,), jnp.int32),
            pltpu.VMEM((2 * VARS, rows, GRID_LON), jnp.float32),
            pltpu.VMEM((rows * BLOCK, LANES), jnp.float32),
            pltpu.SemaphoreType.DMA((rows // 8 + 1,)),
            pltpu.SemaphoreType.DMA((rows // 8,)),
        ],
        compiler_params=pltpu.CompilerParams(vmem_limit_bytes=VMEM_LIMIT),
        name="pack",
    )(in_hbm(valid_mask), in_hbm(ensemble.reshape(2 * VARS, rows, GRID_LON)))
    return packed.reshape(rows, BLOCK // 4, 4, LANES)


def truth_kernel(start_ref, in_ref, truth_ref, weight_ref, near, arrived):
    row = position()
    around = pl.ds(pl.multiple_of((row // 8) * 8, 8), 8)
    look = pltpu.make_async_copy(in_ref.at[:, around, :], near, arrived)
    look.start()
    place = jnp.full((8, LANES), start_ref[0] + row, jnp.int32).astype(jnp.float32)
    angle = (90.0 - place * 180.0 / (GRID_LAT - 1)) * math.pi / 180.0
    weight_ref[...] = jnp.cos(angle)
    mine = lax.broadcasted_iota(jnp.int32, (8, LANES), 0) == row % 8
    look.wait()

    def pick(var, low, high):
        piece = jnp.where(mine[:, : high - low], near[var, :, low:high], 0.0)
        return jnp.sum(piece, axis=0, keepdims=True)

    rows = [
        pick(var, col * LANES, col * LANES + LANES) for var in range(VARS) for col in range(FULL)
    ]
    ends = [pick(var, FULL * LANES, GRID_LON) for var in range(VARS)]
    ends.append(jnp.zeros((1, LANES - VARS * TAIL), jnp.float32))
    rows.append(jnp.concatenate(ends, axis=1))
    for row in range(WHOLE):
        truth_ref[row : row + 1, :] = rows[row]
    for row in range(8):
        truth_ref[WHOLE + row : WHOLE + row + 1, :] = rows[WHOLE + row % 2]


def truth(observation, band_start):
    rows = observation.shape[2]
    return pl.pallas_call(
        truth_kernel,
        in_specs=[
            pl.BlockSpec(memory_space=pltpu.SMEM),
            pl.BlockSpec(memory_space=pltpu.HBM),
        ],
        out_specs=[pl.BlockSpec(memory_space=pltpu.VMEM)] * 2,
        out_shape=[
            jax.ShapeDtypeStruct((40, LANES), jnp.float32),
            jax.ShapeDtypeStruct((8, LANES), jnp.float32),
        ],
        scratch_shapes=[
            pltpu.VMEM((VARS, 8, GRID_LON), jnp.float32),
            pltpu.SemaphoreType.DMA(()),
        ],
        compiler_params=pltpu.CompilerParams(vmem_limit_bytes=VMEM_LIMIT),
        name="truth",
    )(band_start, in_hbm(observation.reshape(VARS, rows, GRID_LON)))


def compare(values, i, j):
    low, high = values[i], values[j]
    values[i] = jnp.minimum(low, high)
    values[j] = jnp.maximum(low, high)


def merge(values, where):
    if len(where) == 2:
        compare(values, where[0], where[1])
        return
    merge(values, where[0::2])
    merge(values, where[1::2])
    for k in range(1, len(where) - 1, 2):
        compare(values, where[k], where[k + 1])


def sort(values, where):
    if len(where) == 1:
        return
    half = len(where) // 2
    sort(values, where[:half])
    sort(values, where[half:])
    merge(values, where)


def score_of(ordered, observed):
    skill = sum(jnp.abs(v - observed) for v in ordered)
    spread = sum(
        (VALID - 1.0 - 2 * k) * (ordered[VALID - 1 - k] - ordered[k]) for k in range(VALID // 2)
    )
    return skill * (1.0 / VALID) - spread * (1.0 / (VALID * (VALID - 1.0)))


def halve(values):
    step = len(values) // 2
    while step:
        for k in range(len(values)):
            if not k & step:
                compare(values, k, k + step)
        step //= 2


def score_rest(parts, observed):
    count = len(parts)
    sublane = lax.broadcasted_iota(jnp.int32, (8, LANES), 0)
    pair = sublane // 2
    odd = pair % 2 == 1
    upper = pair >= 2
    values = list(parts)

    def swap(v, beside):
        up, down = pltpu.roll(v, 2, 0), pltpu.roll(v, 6, 0)
        return jnp.where(odd, up, down) if beside else jnp.where(odd, down, up)

    def split(values, others, high):
        return [
            jnp.where(high, jnp.maximum(v, w), jnp.minimum(v, w)) for v, w in zip(values, others)
        ]

    sort(values, list(range(count)))
    values = split(values, [swap(v, True) for v in values[::-1]], odd)
    halve(values)
    values = split(values, [swap(v, False) for v in values[::-1]], upper)
    values = split(values, [swap(v, True) for v in values], odd)
    halve(values)
    skill = jnp.zeros((8, LANES), jnp.float32)
    spread = jnp.zeros((8, LANES), jnp.float32)
    for k, v in enumerate(values):
        rank = count * pair + k
        v = jnp.where(rank < VALID, v, observed)
        weight = jnp.where(rank < VALID, 2 * rank - (VALID - 1), 0).astype(jnp.float32)
        skill = skill + jnp.abs(v - observed)
        spread = spread + weight * v
    total = skill * (1.0 / VALID) - spread * (1.0 / (VALID * (VALID - 1.0)))
    total = total + pltpu.roll(total, 4, 0)
    return total + pltpu.roll(total, 2, 0)


def score_kernel(weight_ref, in_ref, truth_ref, field_ref, sums_ref, field):
    sources = MEMBERS // 2

    @pl.loop(0, WHOLE // 8)
    def _(tile):
        values = []
        for source in range(sources):
            for member in range(2):
                base = BLOCK * source + 4 * (source % 2) + WHOLE * member
                at = pl.multiple_of(base + tile * 8, 8)
                values.append(in_ref[pl.ds(at, 8), :])
        sort(values, list(range(MEMBERS)))
        start = pl.multiple_of(tile * 8, 8)
        field[pl.ds(start, 8), :] = score_of(values[:VALID], truth_ref[pl.ds(start, 8), :])

    parts = [in_ref[136 * k + 64 : 136 * k + 72, :] for k in range(sources // 2)]
    field[WHOLE : WHOLE + 8, :] = score_rest(parts, truth_ref[WHOLE : WHOLE + 8, :])

    lane = lax.broadcasted_iota(jnp.int32, (1, LANES), 1)
    ends = field[VARS * FULL : VARS * FULL + 1, :]
    sums = jnp.zeros((1, LANES), jnp.float32)
    for var in range(VARS):
        total = jnp.where((lane >= var * TAIL) & (lane < (var + 1) * TAIL), ends, 0.0)
        for col in range(FULL):
            row = field[var * FULL + col : var * FULL + col + 1, :]
            field_ref[var, :, col * LANES : col * LANES + LANES] = row
            total = total + row
        field_ref[var, :, FULL * LANES : GRID_LON] = ends[:, var * TAIL : (var + 1) * TAIL]
        total = jnp.sum(total, axis=1, keepdims=True)
        sums = jnp.where(lane == var, total, sums)
    sums_ref[...] = jnp.broadcast_to(sums * weight_ref[0:1, :], sums_ref.shape)


def score(weight, members, observed, copies):
    return pl.pallas_call(
        score_kernel,
        in_specs=[
            pl.BlockSpec(memory_space=pltpu.VMEM),
            pl.BlockSpec(memory_space=pltpu.VMEM),
            pl.BlockSpec(memory_space=pltpu.VMEM),
        ],
        out_specs=[pl.BlockSpec(memory_space=pltpu.VMEM)] * 2,
        out_shape=[
            jax.ShapeDtypeStruct((VARS, 1, GRID_LON), jnp.float32),
            jax.ShapeDtypeStruct((copies, LANES), jnp.float32),
        ],
        scratch_shapes=[pltpu.VMEM((40, LANES), jnp.float32)],
        compiler_params=pltpu.CompilerParams(vmem_limit_bytes=VMEM_LIMIT),
        name="score",
    )(weight, members, observed)


def finish_kernel(in_ref, ready_ref, table_ref, field_ref, table, sent, *, cells):
    first = pltpu.make_async_copy(ready_ref, field_ref, sent.at[0])
    second = pltpu.make_async_copy(table, table_ref, sent.at[1])
    first.start()
    table[...] = jnp.sum(in_ref[...], axis=0, keepdims=True)[:, :VARS] / cells
    second.start()
    first.wait()
    second.wait()


def finish(sums, field, cells):
    return pl.pallas_call(
        functools.partial(finish_kernel, cells=cells),
        in_specs=[pl.BlockSpec(memory_space=pltpu.VMEM)] * 2,
        out_specs=[pl.BlockSpec(memory_space=pltpu.HBM)] * 2,
        out_shape=[
            jax.ShapeDtypeStruct((1, VARS), jnp.float32),
            jax.ShapeDtypeStruct(field.shape, jnp.float32),
        ],
        scratch_shapes=[pltpu.VMEM((1, VARS), jnp.float32), pltpu.SemaphoreType.DMA((2,))],
        compiler_params=pltpu.CompilerParams(vmem_limit_bytes=VMEM_LIMIT),
        name="finish",
    )(sums, field)


def on_device(ensemble, observation, valid_mask, band_start):
    lat_rows = ensemble.shape[3]
    packed = pack(ensemble, valid_mask)
    members = lax.all_to_all(packed, MEMBER, split_axis=0, concat_axis=0, tiled=True)
    members = members.reshape(-1, LANES)
    observed, weight = truth(observation, band_start)
    field, sums = score(weight, members, observed, lax.axis_size(MEMBER_LAT))
    sums = lax.all_to_all(sums, MEMBER_LAT, split_axis=0, concat_axis=0, tiled=True)
    cells = lax.axis_size("lat") * lat_rows * GRID_LON
    table, field = finish(sums, field, cells)
    return (field.reshape(VARS, 1, 1, GRID_LON), table.reshape(VARS, 1))


def solution(mesh):
    torus = Mesh(
        mesh.devices.reshape(4, 4, 2, mesh.shape["lat"]),
        ("member_0", "member_1", "member_2", "lat"),
    )
    in_specs = (P(MEMBER, None, None, "lat", None), P(None, None, "lat", None), P(MEMBER), P("lat"))
    out_specs = (P(None, None, LAT_MEMBER, None), P())
    return jax.shard_map(
        on_device, mesh=torus, in_specs=in_specs, out_specs=out_specs, check_vma=False
    )
```

```python
import functools
import math

import jax
import jax.numpy as jnp
from jax import lax
from jax.experimental import pallas as pl
from jax.experimental.pallas import tpu as pltpu
from jax.sharding import Mesh
from jax.sharding import PartitionSpec as P

GRID_LAT = 721
GRID_LON = 1440
LANES = 128
VARS = 3
FULL = 11
TAIL = 32
BLOCK = 68
WHOLE = 32
MEMBERS = 64
VALID = 50
VMEM_LIMIT = 8 * 2**20
PAD = 1e30
MEMBER = ("member_0", "member_1", "member_2")
MEMBER_LAT = ("member_2", "member_0", "member_1", "lat")
LAT_MEMBER = ("lat", "member_0", "member_1", "member_2")


def position():
    return lax.axis_index(MEMBER).astype(jnp.int32)


def in_hbm(x):
    return pltpu.with_memory_space_constraint(x, pltpu.HBM)


def pack_kernel(mask_in, in_ref, out_ref, mask_ref, held, packed, arrived, left):
    tiles = held.shape[1] // 8
    depth = 8 * BLOCK
    core = lax.axis_index(MEMBER[2]).astype(jnp.int32)

    def bring(tile):
        rows = pl.ds(tile * 8, 8)
        return pltpu.make_async_copy(
            in_ref.at[:, rows, :], held.at[:, rows, :], arrived.at[tile]
        )

    def take(tile):
        rows = pl.ds(tile * depth, depth)
        return pltpu.make_async_copy(packed.at[rows, :], out_ref.at[rows, :], left.at[tile])

    flags = pltpu.make_async_copy(mask_in, mask_ref, arrived.at[tiles])
    flags.start()
    for tile in range(tiles):
        bring(tile).start()
    flags.wait()
    for tile in range(tiles):
        bring(tile).wait()
        rows = slice(tile * 8, tile * 8 + 8)
        pieces = [[], []]
        for member in range(2):
            valid = mask_ref[member] != 0
            ends = []
            for var in range(VARS):
                for col in range(FULL):
                    low = col * LANES
                    pieces[member].append(held[member * VARS + var, rows, low : low + LANES])
                ends.append(held[member * VARS + var, rows, FULL * LANES : GRID_LON])
            ends.append(jnp.zeros((8, LANES - VARS * TAIL), jnp.float32))
            pieces[member].append(jnp.concatenate(ends, axis=1))
            pieces[member] = [jnp.where(valid, piece, PAD) for piece in pieces[member]]
        for line, pair in enumerate(zip(*pieces)):
            for member, piece in enumerate((jnp.minimum(*pair), jnp.maximum(*pair))):
                if line < WHOLE:
                    start = tile * depth + 4 * core + WHOLE * member + line
                else:
                    start = tile * depth + 64 * (1 - core) + 2 * member + line - WHOLE
                packed[pl.ds(start, 8, stride=BLOCK), :] = piece
        take(tile).start()
    for tile in range(tiles):
        take(tile).wait()


def pack(ensemble, valid_mask):
    rows = ensemble.shape[3]
    packed = pl.pallas_call(
        pack_kernel,
        in_specs=[pl.BlockSpec(memory_space=pltpu.HBM)] * 2,
        out_specs=pl.BlockSpec(memory_space=pltpu.HBM),
        out_shape=jax.ShapeDtypeStruct((rows * BLOCK, LANES), jnp.float32),
        scratch_shapes=[
            pltpu.SMEM((2,), jnp.int32),
            pltpu.VMEM((2 * VARS, rows, GRID_LON), jnp.float32),
            pltpu.VMEM((rows * BLOCK, LANES), jnp.float32),
            pltpu.SemaphoreType.DMA((rows // 8 + 1,)),
            pltpu.SemaphoreType.DMA((rows // 8,)),
        ],
        compiler_params=pltpu.CompilerParams(vmem_limit_bytes=VMEM_LIMIT),
        name="pack",
    )(in_hbm(valid_mask), in_hbm(ensemble.reshape(2 * VARS, rows, GRID_LON)))
    return packed.reshape(rows, BLOCK // 4, 4, LANES)


def truth_kernel(start_ref, in_ref, truth_ref, weight_ref, near, arrived):
    row = position()
    around = pl.ds(pl.multiple_of((row // 8) * 8, 8), 8)
    look = pltpu.make_async_copy(in_ref.at[:, around, :], near, arrived)
    look.start()
    place = jnp.full((8, LANES), start_ref[0] + row, jnp.int32).astype(jnp.float32)
    angle = (90.0 - place * 180.0 / (GRID_LAT - 1)) * math.pi / 180.0
    weight_ref[...] = jnp.cos(angle)
    mine = lax.broadcasted_iota(jnp.int32, (8, LANES), 0) == row % 8
    look.wait()

    def pick(var, low, high):
        piece = jnp.where(mine[:, : high - low], near[var, :, low:high], 0.0)
        return jnp.sum(piece, axis=0, keepdims=True)

    rows = [
        pick(var, col * LANES, col * LANES + LANES) for var in range(VARS) for col in range(FULL)
    ]
    ends = [pick(var, FULL * LANES, GRID_LON) for var in range(VARS)]
    ends.append(jnp.zeros((1, LANES - VARS * TAIL), jnp.float32))
    rows.append(jnp.concatenate(ends, axis=1))
    for row in range(WHOLE):
        truth_ref[row : row + 1, :] = rows[row]
    for row in range(8):
        truth_ref[WHOLE + row : WHOLE + row + 1, :] = rows[WHOLE + row % 2]


def truth(observation, band_start):
    rows = observation.shape[2]
    return pl.pallas_call(
        truth_kernel,
        in_specs=[
            pl.BlockSpec(memory_space=pltpu.SMEM),
            pl.BlockSpec(memory_space=pltpu.HBM),
        ],
        out_specs=[pl.BlockSpec(memory_space=pltpu.VMEM)] * 2,
        out_shape=[
            jax.ShapeDtypeStruct((40, LANES), jnp.float32),
            jax.ShapeDtypeStruct((8, LANES), jnp.float32),
        ],
        scratch_shapes=[
            pltpu.VMEM((VARS, 8, GRID_LON), jnp.float32),
            pltpu.SemaphoreType.DMA(()),
        ],
        compiler_params=pltpu.CompilerParams(vmem_limit_bytes=VMEM_LIMIT),
        name="truth",
    )(band_start, in_hbm(observation.reshape(VARS, rows, GRID_LON)))


def compare(values, i, j):
    low, high = values[i], values[j]
    values[i] = jnp.minimum(low, high)
    values[j] = jnp.maximum(low, high)


def merge(values, where):
    if len(where) == 2:
        compare(values, where[0], where[1])
        return
    merge(values, where[0::2])
    merge(values, where[1::2])
    for k in range(1, len(where) - 1, 2):
        compare(values, where[k], where[k + 1])


def sort(values, where, paired=False):
    if len(where) == 1 or (paired and len(where) == 2):
        return
    half = len(where) // 2
    sort(values, where[:half], paired)
    sort(values, where[half:], paired)
    merge(values, where)


def score_of(ordered, observed):
    skill = sum(jnp.abs(v - observed) for v in ordered)
    spread = sum(
        (VALID - 1.0 - 2 * k) * (ordered[VALID - 1 - k] - ordered[k]) for k in range(VALID // 2)
    )
    return skill * (1.0 / VALID) - spread * (1.0 / (VALID * (VALID - 1.0)))


def halve(values):
    step = len(values) // 2
    while step:
        for k in range(len(values)):
            if not k & step:
                compare(values, k, k + step)
        step //= 2


def score_rest(parts, observed):
    count = len(parts)
    sublane = lax.broadcasted_iota(jnp.int32, (8, LANES), 0)
    pair = sublane // 2
    odd = pair % 2 == 1
    upper = pair >= 2
    values = list(parts)

    def swap(v, beside):
        up, down = pltpu.roll(v, 2, 0), pltpu.roll(v, 6, 0)
        return jnp.where(odd, up, down) if beside else jnp.where(odd, down, up)

    def split(values, others, high):
        return [
            jnp.where(high, jnp.maximum(v, w), jnp.minimum(v, w)) for v, w in zip(values, others)
        ]

    sort(values, list(range(count)))
    values = split(values, [swap(v, True) for v in values[::-1]], odd)
    halve(values)
    values = split(values, [swap(v, False) for v in values[::-1]], upper)
    values = split(values, [swap(v, True) for v in values], odd)
    halve(values)
    skill = jnp.zeros((8, LANES), jnp.float32)
    spread = jnp.zeros((8, LANES), jnp.float32)
    for k, v in enumerate(values):
        rank = count * pair + k
        v = jnp.where(rank < VALID, v, observed)
        weight = jnp.where(rank < VALID, 2 * rank - (VALID - 1), 0).astype(jnp.float32)
        skill = skill + jnp.abs(v - observed)
        spread = spread + weight * v
    total = skill * (1.0 / VALID) - spread * (1.0 / (VALID * (VALID - 1.0)))
    total = total + pltpu.roll(total, 4, 0)
    return total + pltpu.roll(total, 2, 0)


def score_kernel(weight_ref, in_ref, truth_ref, field_ref, sums_ref, field):
    sources = MEMBERS // 2

    @pl.loop(0, WHOLE // 8)
    def _(tile):
        values = []
        for source in range(sources):
            for member in range(2):
                base = BLOCK * source + 4 * (source % 2) + WHOLE * member
                at = pl.multiple_of(base + tile * 8, 8)
                values.append(in_ref[pl.ds(at, 8), :])
        sort(values, list(range(MEMBERS)), paired=True)
        start = pl.multiple_of(tile * 8, 8)
        field[pl.ds(start, 8), :] = score_of(values[:VALID], truth_ref[pl.ds(start, 8), :])

    parts = [in_ref[136 * k + 64 : 136 * k + 72, :] for k in range(sources // 2)]
    field[WHOLE : WHOLE + 8, :] = score_rest(parts, truth_ref[WHOLE : WHOLE + 8, :])

    lane = lax.broadcasted_iota(jnp.int32, (1, LANES), 1)
    ends = field[VARS * FULL : VARS * FULL + 1, :]
    sums = jnp.zeros((1, LANES), jnp.float32)
    for var in range(VARS):
        total = jnp.where((lane >= var * TAIL) & (lane < (var + 1) * TAIL), ends, 0.0)
        for col in range(FULL):
            row = field[var * FULL + col : var * FULL + col + 1, :]
            field_ref[var, :, col * LANES : col * LANES + LANES] = row
            total = total + row
        field_ref[var, :, FULL * LANES : GRID_LON] = ends[:, var * TAIL : (var + 1) * TAIL]
        total = jnp.sum(total, axis=1, keepdims=True)
        sums = jnp.where(lane == var, total, sums)
    sums_ref[...] = jnp.broadcast_to(sums * weight_ref[0:1, :], sums_ref.shape)


def score(weight, members, observed, copies):
    return pl.pallas_call(
        score_kernel,
        in_specs=[
            pl.BlockSpec(memory_space=pltpu.VMEM),
            pl.BlockSpec(memory_space=pltpu.VMEM),
            pl.BlockSpec(memory_space=pltpu.VMEM),
        ],
        out_specs=[pl.BlockSpec(memory_space=pltpu.VMEM)] * 2,
        out_shape=[
            jax.ShapeDtypeStruct((VARS, 1, GRID_LON), jnp.float32),
            jax.ShapeDtypeStruct((copies, LANES), jnp.float32),
        ],
        scratch_shapes=[pltpu.VMEM((40, LANES), jnp.float32)],
        compiler_params=pltpu.CompilerParams(vmem_limit_bytes=VMEM_LIMIT,
        ),
        name="score",
    )(weight, members, observed)


def finish_kernel(in_ref, ready_ref, table_ref, field_ref, table, sent, *, cells):
    first = pltpu.make_async_copy(ready_ref, field_ref, sent.at[0])
    second = pltpu.make_async_copy(table, table_ref, sent.at[1])
    first.start()
    table[...] = jnp.sum(in_ref[...], axis=0, keepdims=True)[:, :VARS] / cells
    second.start()
    first.wait()
    second.wait()


def finish(sums, field, cells):
    return pl.pallas_call(
        functools.partial(finish_kernel, cells=cells),
        in_specs=[pl.BlockSpec(memory_space=pltpu.VMEM)] * 2,
        out_specs=[pl.BlockSpec(memory_space=pltpu.HBM)] * 2,
        out_shape=[
            jax.ShapeDtypeStruct((1, VARS), jnp.float32),
            jax.ShapeDtypeStruct(field.shape, jnp.float32),
        ],
        scratch_shapes=[pltpu.VMEM((1, VARS), jnp.float32), pltpu.SemaphoreType.DMA((2,))],
        compiler_params=pltpu.CompilerParams(vmem_limit_bytes=VMEM_LIMIT),
        name="finish",
    )(sums, field)


def on_device(ensemble, observation, valid_mask, band_start):
    lat_rows = ensemble.shape[3]
    packed = pack(ensemble, valid_mask)
    members = lax.all_to_all(packed, MEMBER, split_axis=0, concat_axis=0, tiled=True)
    members = members.reshape(-1, LANES)
    observed, weight = truth(observation, band_start)
    field, sums = score(weight, members, observed, lax.axis_size(MEMBER_LAT))
    sums = lax.all_to_all(sums, MEMBER_LAT, split_axis=0, concat_axis=0, tiled=True)
    cells = lax.axis_size("lat") * lat_rows * GRID_LON
    table, field = finish(sums, field, cells)
    return (field.reshape(VARS, 1, 1, GRID_LON), table.reshape(VARS, 1))


def solution(mesh):
    torus = Mesh(
        mesh.devices.reshape(4, 4, 2, mesh.shape["lat"]),
        ("member_0", "member_1", "member_2", "lat"),
    )
    in_specs = (P(MEMBER, None, None, "lat", None), P(None, None, "lat", None), P(MEMBER), P("lat"))
    out_specs = (P(None, None, LAT_MEMBER, None), P())
    return jax.shard_map(
        on_device, mesh=torus, in_specs=in_specs, out_specs=out_specs, check_vma=False
    )
```

```python
import functools
import math

import jax
import jax.numpy as jnp
from jax import lax
from jax.experimental import pallas as pl
from jax.experimental.pallas import tpu as pltpu
from jax.sharding import Mesh
from jax.sharding import PartitionSpec as P

GRID_LAT = 721
GRID_LON = 1440
LANES = 128
VARS = 3
FULL = 11
TAIL = 32
BLOCK = 68
WHOLE = 32
MEMBERS = 64
VALID = 50
VMEM_LIMIT = 8 * 2**20
PAD = 1e30
MEMBER = ("member_0", "member_1", "member_2")
MEMBER_LAT = ("member_2", "member_1", "member_0", "lat")
LAT_MEMBER = ("lat", "member_0", "member_1", "member_2")


def position():
    return lax.axis_index(MEMBER).astype(jnp.int32)


def in_hbm(x):
    return pltpu.with_memory_space_constraint(x, pltpu.HBM)


def pack_kernel(mask_in, in_ref, out_ref, mask_ref, held, packed, arrived, left):
    tiles = held.shape[1] // 8
    depth = 8 * BLOCK
    core = lax.axis_index(MEMBER[2]).astype(jnp.int32)

    def bring(tile):
        rows = pl.ds(tile * 8, 8)
        return pltpu.make_async_copy(
            in_ref.at[:, rows, :], held.at[:, rows, :], arrived.at[tile]
        )

    def take(tile):
        rows = pl.ds(tile * depth, depth)
        return pltpu.make_async_copy(packed.at[rows, :], out_ref.at[rows, :], left.at[tile])

    flags = pltpu.make_async_copy(mask_in, mask_ref, arrived.at[tiles])
    flags.start()
    for tile in range(tiles):
        bring(tile).start()
    flags.wait()
    for tile in range(tiles):
        bring(tile).wait()
        rows = slice(tile * 8, tile * 8 + 8)
        pieces = [[], []]
        for member in range(2):
            valid = mask_ref[member] != 0
            ends = []
            for var in range(VARS):
                for col in range(FULL):
                    low = col * LANES
                    pieces[member].append(held[member * VARS + var, rows, low : low + LANES])
                ends.append(held[member * VARS + var, rows, FULL * LANES : GRID_LON])
            ends.append(jnp.zeros((8, LANES - VARS * TAIL), jnp.float32))
            pieces[member].append(jnp.concatenate(ends, axis=1))
            pieces[member] = [jnp.where(valid, piece, PAD) for piece in pieces[member]]
        for line, pair in enumerate(zip(*pieces)):
            for member, piece in enumerate((jnp.minimum(*pair), jnp.maximum(*pair))):
                if line < WHOLE:
                    start = tile * depth + 4 * core + WHOLE * member + line
                else:
                    start = tile * depth + 64 * (1 - core) + 2 * member + line - WHOLE
                packed[pl.ds(start, 8, stride=BLOCK), :] = piece
        take(tile).start()
    for tile in range(tiles):
        take(tile).wait()


def pack(ensemble, valid_mask):
    rows = ensemble.shape[3]
    packed = pl.pallas_call(
        pack_kernel,
        in_specs=[pl.BlockSpec(memory_space=pltpu.HBM)] * 2,
        out_specs=pl.BlockSpec(memory_space=pltpu.HBM),
        out_shape=jax.ShapeDtypeStruct((rows * BLOCK, LANES), jnp.float32),
        scratch_shapes=[
            pltpu.SMEM((2,), jnp.int32),
            pltpu.VMEM((2 * VARS, rows, GRID_LON), jnp.float32),
            pltpu.VMEM((rows * BLOCK, LANES), jnp.float32),
            pltpu.SemaphoreType.DMA((rows // 8 + 1,)),
            pltpu.SemaphoreType.DMA((rows // 8,)),
        ],
        compiler_params=pltpu.CompilerParams(vmem_limit_bytes=VMEM_LIMIT),
        name="pack",
    )(in_hbm(valid_mask), in_hbm(ensemble.reshape(2 * VARS, rows, GRID_LON)))
    return packed.reshape(rows, BLOCK // 4, 4, LANES)


def truth_kernel(start_ref, in_ref, truth_ref, weight_ref, near, arrived):
    row = position()
    around = pl.ds(pl.multiple_of((row // 8) * 8, 8), 8)
    look = pltpu.make_async_copy(in_ref.at[:, around, :], near, arrived)
    look.start()
    place = jnp.full((8, LANES), start_ref[0] + row, jnp.int32).astype(jnp.float32)
    angle = (90.0 - place * 180.0 / (GRID_LAT - 1)) * math.pi / 180.0
    weight_ref[...] = jnp.cos(angle)
    mine = lax.broadcasted_iota(jnp.int32, (8, LANES), 0) == row % 8
    look.wait()

    def pick(var, low, high):
        piece = jnp.where(mine[:, : high - low], near[var, :, low:high], 0.0)
        return jnp.sum(piece, axis=0, keepdims=True)

    rows = [
        pick(var, col * LANES, col * LANES + LANES) for var in range(VARS) for col in range(FULL)
    ]
    ends = [pick(var, FULL * LANES, GRID_LON) for var in range(VARS)]
    ends.append(jnp.zeros((1, LANES - VARS * TAIL), jnp.float32))
    rows.append(jnp.concatenate(ends, axis=1))
    for row in range(WHOLE):
        truth_ref[row : row + 1, :] = rows[row]
    for row in range(8):
        truth_ref[WHOLE + row : WHOLE + row + 1, :] = rows[WHOLE + row % 2]


def truth(observation, band_start):
    rows = observation.shape[2]
    return pl.pallas_call(
        truth_kernel,
        in_specs=[
            pl.BlockSpec(memory_space=pltpu.SMEM),
            pl.BlockSpec(memory_space=pltpu.HBM),
        ],
        out_specs=[pl.BlockSpec(memory_space=pltpu.VMEM)] * 2,
        out_shape=[
            jax.ShapeDtypeStruct((40, LANES), jnp.float32),
            jax.ShapeDtypeStruct((8, LANES), jnp.float32),
        ],
        scratch_shapes=[
            pltpu.VMEM((VARS, 8, GRID_LON), jnp.float32),
            pltpu.SemaphoreType.DMA(()),
        ],
        compiler_params=pltpu.CompilerParams(vmem_limit_bytes=VMEM_LIMIT),
        name="truth",
    )(band_start, in_hbm(observation.reshape(VARS, rows, GRID_LON)))


def compare(values, i, j):
    low, high = values[i], values[j]
    values[i] = jnp.minimum(low, high)
    values[j] = jnp.maximum(low, high)


def merge(values, where):
    if len(where) == 2:
        compare(values, where[0], where[1])
        return
    merge(values, where[0::2])
    merge(values, where[1::2])
    for k in range(1, len(where) - 1, 2):
        compare(values, where[k], where[k + 1])


def sort(values, where, paired=False):
    if len(where) == 1 or (paired and len(where) == 2):
        return
    half = len(where) // 2
    sort(values, where[:half], paired)
    sort(values, where[half:], paired)
    merge(values, where)


def score_of(ordered, observed):
    skill = sum(jnp.abs(v - observed) for v in ordered)
    spread = sum(
        (VALID - 1.0 - 2 * k) * (ordered[VALID - 1 - k] - ordered[k]) for k in range(VALID // 2)
    )
    return skill * (1.0 / VALID) - spread * (1.0 / (VALID * (VALID - 1.0)))


def halve(values):
    step = len(values) // 2
    while step:
        for k in range(len(values)):
            if not k & step:
                compare(values, k, k + step)
        step //= 2


def score_rest(parts, observed):
    count = len(parts)
    sublane = lax.broadcasted_iota(jnp.int32, (8, LANES), 0)
    pair = sublane // 2
    odd = pair % 2 == 1
    upper = pair >= 2
    values = list(parts)

    def swap(v, beside):
        up, down = pltpu.roll(v, 2, 0), pltpu.roll(v, 6, 0)
        return jnp.where(odd, up, down) if beside else jnp.where(odd, down, up)

    def split(values, others, high):
        return [
            jnp.where(high, jnp.maximum(v, w), jnp.minimum(v, w)) for v, w in zip(values, others)
        ]

    sort(values, list(range(count)))
    values = split(values, [swap(v, True) for v in values[::-1]], odd)
    halve(values)
    values = split(values, [swap(v, False) for v in values[::-1]], upper)
    values = split(values, [swap(v, True) for v in values], odd)
    halve(values)
    skill = jnp.zeros((8, LANES), jnp.float32)
    spread = jnp.zeros((8, LANES), jnp.float32)
    for k, v in enumerate(values):
        rank = count * pair + k
        v = jnp.where(rank < VALID, v, observed)
        weight = jnp.where(rank < VALID, 2 * rank - (VALID - 1), 0).astype(jnp.float32)
        skill = skill + jnp.abs(v - observed)
        spread = spread + weight * v
    total = skill * (1.0 / VALID) - spread * (1.0 / (VALID * (VALID - 1.0)))
    total = total + pltpu.roll(total, 4, 0)
    return total + pltpu.roll(total, 2, 0)


def score_kernel(weight_ref, in_ref, truth_ref, field_ref, sums_ref, field):
    sources = MEMBERS // 2

    @pl.loop(0, WHOLE // 8)
    def _(tile):
        values = []
        for source in range(sources):
            for member in range(2):
                base = BLOCK * source + 4 * (source % 2) + WHOLE * member
                at = pl.multiple_of(base + tile * 8, 8)
                values.append(in_ref[pl.ds(at, 8), :])
        sort(values, list(range(MEMBERS)), paired=True)
        start = pl.multiple_of(tile * 8, 8)
        field[pl.ds(start, 8), :] = score_of(values[:VALID], truth_ref[pl.ds(start, 8), :])

    parts = [in_ref[136 * k + 64 : 136 * k + 72, :] for k in range(sources // 2)]
    field[WHOLE : WHOLE + 8, :] = score_rest(parts, truth_ref[WHOLE : WHOLE + 8, :])

    lane = lax.broadcasted_iota(jnp.int32, (1, LANES), 1)
    ends = field[VARS * FULL : VARS * FULL + 1, :]
    sums = jnp.zeros((1, LANES), jnp.float32)
    for var in range(VARS):
        total = jnp.where((lane >= var * TAIL) & (lane < (var + 1) * TAIL), ends, 0.0)
        for col in range(FULL):
            row = field[var * FULL + col : var * FULL + col + 1, :]
            field_ref[var, :, col * LANES : col * LANES + LANES] = row
            total = total + row
        field_ref[var, :, FULL * LANES : GRID_LON] = ends[:, var * TAIL : (var + 1) * TAIL]
        total = jnp.sum(total, axis=1, keepdims=True)
        sums = jnp.where(lane == var, total, sums)
    sums_ref[...] = jnp.broadcast_to(sums * weight_ref[0:1, :], sums_ref.shape)


def score(weight, members, observed, copies):
    return pl.pallas_call(
        score_kernel,
        in_specs=[
            pl.BlockSpec(memory_space=pltpu.VMEM),
            pl.BlockSpec(memory_space=pltpu.VMEM),
            pl.BlockSpec(memory_space=pltpu.VMEM),
        ],
        out_specs=[pl.BlockSpec(memory_space=pltpu.VMEM)] * 2,
        out_shape=[
            jax.ShapeDtypeStruct((VARS, 1, GRID_LON), jnp.float32),
            jax.ShapeDtypeStruct((copies, LANES), jnp.float32),
        ],
        scratch_shapes=[pltpu.VMEM((40, LANES), jnp.float32)],
        compiler_params=pltpu.CompilerParams(vmem_limit_bytes=VMEM_LIMIT,
        ),
        name="score",
    )(weight, members, observed)


def finish_kernel(in_ref, ready_ref, table_ref, field_ref, table, sent, *, cells):
    first = pltpu.make_async_copy(ready_ref, field_ref, sent.at[0])
    second = pltpu.make_async_copy(table, table_ref, sent.at[1])
    first.start()
    table[...] = jnp.sum(in_ref[...], axis=0, keepdims=True)[:, :VARS] / cells
    second.start()
    first.wait()
    second.wait()


def finish(sums, field, cells):
    return pl.pallas_call(
        functools.partial(finish_kernel, cells=cells),
        in_specs=[pl.BlockSpec(memory_space=pltpu.VMEM)] * 2,
        out_specs=[pl.BlockSpec(memory_space=pltpu.HBM)] * 2,
        out_shape=[
            jax.ShapeDtypeStruct((1, VARS), jnp.float32),
            jax.ShapeDtypeStruct(field.shape, jnp.float32),
        ],
        scratch_shapes=[pltpu.VMEM((1, VARS), jnp.float32), pltpu.SemaphoreType.DMA((2,))],
        compiler_params=pltpu.CompilerParams(vmem_limit_bytes=VMEM_LIMIT),
        name="finish",
    )(sums, field)


def on_device(ensemble, observation, valid_mask, band_start):
    lat_rows = ensemble.shape[3]
    packed = pack(ensemble, valid_mask)
    members = lax.all_to_all(packed, MEMBER, split_axis=0, concat_axis=0, tiled=True)
    members = members.reshape(-1, LANES)
    observed, weight = truth(observation, band_start)
    field, sums = score(weight, members, observed, lax.axis_size(MEMBER_LAT))
    sums = lax.all_to_all(sums, MEMBER_LAT, split_axis=0, concat_axis=0, tiled=True)
    cells = lax.axis_size("lat") * lat_rows * GRID_LON
    table, field = finish(sums, field, cells)
    return (field.reshape(VARS, 1, 1, GRID_LON), table.reshape(VARS, 1))


def solution(mesh):
    torus = Mesh(
        mesh.devices.reshape(4, 4, 2, mesh.shape["lat"]),
        ("member_0", "member_1", "member_2", "lat"),
    )
    in_specs = (P(MEMBER, None, None, "lat", None), P(None, None, "lat", None), P(MEMBER), P("lat"))
    out_specs = (P(None, None, LAT_MEMBER, None), P())
    return jax.shard_map(
        on_device, mesh=torus, in_specs=in_specs, out_specs=out_specs, check_vma=False
    )
```
